32 devices in a mesh: head: 2 (over y), seq: 16 (over z, x, core).
Axes of the slice: x: 2, y: 2, z: 4, core: 2. Of those that a mesh axis runs over, the one named last changes fastest.
Arguments:
- queries: bfloat16 [2048, 4096], P(('seq', 'head')), may hold values from -20 to 20
- keys: bfloat16 [2048, 1024], P(('seq', 'head')), may hold values from -5 to 5
- values: bfloat16 [2048, 1024], P(('seq', 'head')), may hold values from -6 to 6
Outputs:
- attended: bfloat16 [2048, 4096], P(('seq', 'head'))
The draws below stay inside these ranges and needn't reach their ends.
All inputs are finite; a program needn't handle non-finite values.
Results may differ from the reference program's by a relative error of at most 0.0041.
Values may be sent and summed in bfloat16 or wider, within the bound.
No kernel may reach another device: no remote copies, remote signals or barrier semaphores. Data moves between devices by JAX's collectives and lax.ppermute only.
A program may use at most 64 MiB of HBM per device.

```python
import math
import jax
import jax.numpy as jnp
from jax import lax

QHEADS = 32
KV_HEADS = 8
HEAD_DIM = 128
SEQ = 2048


def drawn_pair(key):
    width_q = QHEADS * HEAD_DIM
    width_k = KV_HEADS * HEAD_DIM
    key_q = jax.random.fold_in(key, 101)
    key_k = jax.random.fold_in(key, 102)
    q_draw = jnp.clip(jax.random.normal(key_q, (SEQ, width_q), jnp.float32), -5.0, 5.0)
    k_draw = jnp.clip(jax.random.normal(key_k, (SEQ, width_k), jnp.float32), -5.0, 5.0)
    return (q_draw, k_draw)


def draw_queries(key, part):
    return drawn_pair(key)[0].astype(jnp.bfloat16)


def draw_keys(key, part):
    return drawn_pair(key)[1].astype(jnp.bfloat16)


def block_scale(own_key, extent, shards, smallest, top_value):
    def one(dim, shards_of):
        draws = jax.random.uniform(jax.random.fold_in(jax.random.fold_in(own_key, 6), dim), (shards_of,), jnp.float32, smallest / len(shards), top_value / len(shards))
        return jnp.repeat(jnp.exp(draws), extent[dim] // shards_of).reshape((-1,) + (1,) * (len(extent) - dim - 1))

    factor_of = one(*shards[0])
    for cut in shards[1:]:
        factor_of = factor_of * one(*cut)
    return factor_of


def bell_draw(rng, dims, scale, reach, pieces=(), kind=jnp.bfloat16):
    factor_of = block_scale(rng, dims, pieces, -0.22, 0.18) if pieces else 1.0
    values = jax.random.normal(rng, dims, jnp.float32) * scale * factor_of
    return jnp.minimum(jnp.maximum(values, -reach), reach).astype(kind)


def setup_inputs(seed: int = 0) -> dict:
    arg_keys = jax.random.split(jax.random.key(seed), 4)
    queries = draw_queries(jax.random.fold_in(arg_keys[3], 71), 0)
    keys = draw_keys(jax.random.fold_in(arg_keys[3], 71), 0)
    values = bell_draw(arg_keys[2], (SEQ, KV_HEADS * HEAD_DIM), 1.0, 6.0, ((0, 32),))
    return dict(queries=queries, keys=keys, values=values)


def attend_block(query_rows, query_pos, key_all, value_all, key_pos):
    rows = query_rows.shape[0]
    group = QHEADS // KV_HEADS
    qf = query_rows.astype(jnp.float32).reshape(rows, KV_HEADS, group, HEAD_DIM)
    score = jnp.einsum('tkgd,pkd->tkgp', qf, key_all) / math.sqrt(HEAD_DIM)
    allowed = (key_pos[None, :] <= query_pos[:, None])[:, None, None, :]
    score = jnp.where(allowed, score, jnp.float32(-1e+30))
    largest = lax.optimization_barrier(jnp.max(score, axis=-1, keepdims=True))
    weight = jnp.where(allowed, jnp.exp(score - largest), jnp.float32(0.0))
    total = lax.optimization_barrier(jnp.sum(weight, axis=-1))
    rounded = lax.optimization_barrier(weight.astype(jnp.bfloat16)).astype(jnp.float32)
    summed = jnp.einsum('tkgp,pkd->tkgd', rounded, value_all)
    result = summed / total[..., None]
    return result.reshape(rows, QHEADS * HEAD_DIM).astype(jnp.bfloat16)

def reference(queries, keys, values):
    key_all = keys.astype(jnp.float32).reshape(SEQ, KV_HEADS, HEAD_DIM)
    value_all = values.astype(jnp.float32).reshape(SEQ, KV_HEADS, HEAD_DIM)
    segment = SEQ // 8
    block = math.gcd(segment, 128)
    outputs = []
    for part_index in range(8):
        limit = (part_index + 1) * segment
        key_pos = jnp.arange(limit, dtype=jnp.int32)
        rows = queries[part_index * segment:limit].reshape(segment // block, block, QHEADS * HEAD_DIM)
        positions = (part_index * segment + jnp.arange(segment, dtype=jnp.int32)).reshape(segment // block, block)

        def one_block(pair):
            return attend_block(pair[0], pair[1], key_all[:limit], value_all[:limit], key_pos)
        result = lax.map(one_block, (rows, positions))
        outputs.append(result.reshape(segment, QHEADS * HEAD_DIM))
    return jnp.concatenate(outputs, axis=0)
```

```python
import functools
import math

import jax
import jax.numpy as jnp
from jax import lax
from jax.experimental import pallas as pl
from jax.experimental.pallas import tpu as pltpu
from jax.sharding import Mesh, PartitionSpec as P

HEAD_DIM = 128
SCALE = math.log2(math.e) / math.sqrt(HEAD_DIM)
DIMS_NT = (((1,), (1,)), ((), ()))


def attend_kernel(plane_ref, q_ref, kv_ref, out_ref, *, block):
    plane = plane_ref[0]
    tile = q_ref.shape[0]
    row_block = pl.program_id(0)
    q = q_ref[...]

    def step(start, width, state, masked):
        largest, total, summed = state
        k = kv_ref[pl.ds(start, width), :HEAD_DIM]
        v = kv_ref[pl.ds(start, width), HEAD_DIM:]
        score = lax.dot_general(q, k, DIMS_NT, preferred_element_type=jnp.float32)
        if masked:
            row = lax.broadcasted_iota(jnp.int32, score.shape, 0)
            col = lax.broadcasted_iota(jnp.int32, score.shape, 1)
            score = jnp.where(col <= row + row_block * tile, score, jnp.float32(-1e30))
        new_largest = jnp.maximum(largest, jnp.max(score, axis=1, keepdims=True))
        weight = jnp.exp2((score - new_largest) * SCALE)
        fade = jnp.exp2((largest - new_largest) * SCALE)
        total = total * fade + jnp.sum(weight, axis=1, keepdims=True)
        summed = summed * fade + jnp.dot(
            weight.astype(jnp.bfloat16), v, preferred_element_type=jnp.float32
        )
        return new_largest, total, summed

    state = (
        jnp.full((tile, 1), -1e30, jnp.float32),
        jnp.zeros((tile, 1), jnp.float32),
        jnp.zeros((tile, HEAD_DIM), jnp.float32),
    )
    state = step(pl.multiple_of(plane * block, block), block, state, True)
    state = lax.fori_loop(
        0, plane, lambda i, s: step(pl.multiple_of(i * block, block), block, s, False), state
    )
    out_ref[...] = (state[2] / state[1]).astype(jnp.bfloat16)


def attend(plane, queries, kv):
    rows, width = queries.shape
    keys = kv.shape[0]
    block = rows
    tile = min(rows, 256)
    return pl.pallas_call(
        functools.partial(attend_kernel, block=block),
        grid=(rows // tile, width // HEAD_DIM),
        in_specs=[
            pl.BlockSpec(memory_space=pltpu.SMEM),
            pl.BlockSpec((tile, HEAD_DIM), lambda r, h: (r, h)),
            pl.BlockSpec((keys, 2 * HEAD_DIM), lambda r, h: (0, 0)),
        ],
        out_specs=pl.BlockSpec((tile, HEAD_DIM), lambda r, h: (r, h)),
        out_shape=jax.ShapeDtypeStruct((rows, width), jnp.bfloat16),
        name="attend",
    )(plane, queries, kv)


def on_device(queries, keys, values, *, outer, groups):
    rows = queries.shape[0]
    plane = lax.axis_index("outer")
    paired = jnp.concatenate(
        [keys.reshape(rows, groups, -1), values.reshape(rows, groups, -1)], axis=2
    ).reshape(rows, -1)
    axes = ("inner", "head")
    kv_own = lax.all_to_all(paired, axes, split_axis=1, concat_axis=0, tiled=True)
    q_own = lax.all_to_all(queries, axes, split_axis=1, concat_axis=0, tiled=True)
    if outer <= 8:
        block = kv_own.shape[0]
        kv = jnp.zeros((outer * block, kv_own.shape[1]), kv_own.dtype)
        kv = lax.dynamic_update_slice(kv, kv_own, (plane * block, 0))
        for shift in range(1, outer):
            moved = lax.ppermute(kv_own, "outer", [(i, i + shift) for i in range(outer - shift)])
            source = jnp.where(plane >= shift, plane - shift, plane - shift + outer)
            kv = lax.dynamic_update_slice(kv, moved, (source * block, 0))
    else:
        kv = lax.all_gather(kv_own, "outer", axis=0, tiled=True)
    out = attend(plane.reshape(1).astype(jnp.int32), q_own, kv)
    return lax.all_to_all(out, axes, split_axis=0, concat_axis=1, tiled=True)


def solution(mesh):
    def run(queries, keys, values):
        head, seq = mesh.shape["head"], mesh.shape["seq"]
        inner = math.gcd(seq, max(1, keys.shape[1] // HEAD_DIM // head))
        outer = seq // inner
        split = Mesh(mesh.devices.reshape(head, outer, inner), ("head", "outer", "inner"))
        spec = P(("outer", "inner", "head"), None)
        return jax.shard_map(
            functools.partial(on_device, outer=outer, groups=head * inner),
            mesh=split,
            in_specs=(spec, spec, spec),
            out_specs=spec,
            check_vma=False,
        )(queries, keys, values)

    return run
```

```python
import functools
import math

import jax
import jax.numpy as jnp
from jax import lax
from jax.experimental import pallas as pl
from jax.experimental.pallas import tpu as pltpu
from jax.sharding import Mesh, PartitionSpec as P

HEAD_DIM = 128
SCALE = math.log2(math.e) / math.sqrt(HEAD_DIM)
DIMS_NT = (((1,), (1,)), ((), ()))
VMEM_LIMIT = 48 * 1024 * 1024


def scores(q, k):
    return lax.dot_general(q, k, DIMS_NT, preferred_element_type=jnp.float32)


def weigh(score, largest):
    weight = jnp.exp2((score - largest) * SCALE)
    return jnp.sum(weight, axis=1, keepdims=True), weight.astype(jnp.bfloat16)


def stack_heads(ref, start, rows):
    group = ref.shape[1] // HEAD_DIM
    return jnp.concatenate(
        [ref[pl.ds(start, rows), h * HEAD_DIM : (h + 1) * HEAD_DIM] for h in range(group)], axis=0
    )


def pack_state(largest, total, rows):
    lane = lax.broadcasted_iota(jnp.int32, (rows, HEAD_DIM), 1)
    return jnp.where(lane < HEAD_DIM // 2, largest, total)


def own_kernel(core_ref, q_ref, own_ref, other_ref, summed_ref, state_ref, *, run):
    group = q_ref.shape[1] // HEAD_DIM
    tall = group * run
    row = lax.broadcasted_iota(jnp.int32, (tall, run), 0) % run
    col = lax.broadcasted_iota(jnp.int32, (tall, run), 1)
    low = jnp.float32(-1e30)
    see_other = lax.broadcast(core_ref[0], (tall, run)) > 0
    for i in range(q_ref.shape[0] // run):
        q = stack_heads(q_ref, i * run, run)
        own = scores(q, own_ref[: (i + 1) * run, :HEAD_DIM])
        other = scores(q, other_ref[: (i + 1) * run, :HEAD_DIM])
        own_edge = jnp.where(col <= row, own[:, i * run :], low)
        other_edge = jnp.where(see_other, other[:, i * run :], low)
        if i:
            own_edge = jnp.concatenate([own[:, : i * run], own_edge], axis=1)
            other_edge = jnp.concatenate([other[:, : i * run], other_edge], axis=1)
        largest = jnp.maximum(
            jnp.max(own_edge, axis=1, keepdims=True), jnp.max(other_edge, axis=1, keepdims=True)
        )
        own_total, own_weight = weigh(own_edge, largest)
        other_total, other_weight = weigh(other_edge, largest)
        summed_ref[i * tall : (i + 1) * tall, :] = jnp.dot(
            own_weight, own_ref[: (i + 1) * run, HEAD_DIM:], preferred_element_type=jnp.float32
        ) + jnp.dot(
            other_weight, other_ref[: (i + 1) * run, HEAD_DIM:], preferred_element_type=jnp.float32
        )
        state_ref[i * tall : (i + 1) * tall, :] = pack_state(
            largest, own_total + other_total, tall
        )


def earlier_kernel(count_ref, q_ref, kv_ref, summed_in, state_in, *outs, run, last):
    group = q_ref.shape[1] // HEAD_DIM
    tall = group * run
    runs = q_ref.shape[0] // run
    half = HEAD_DIM // 2
    count = count_ref[0]

    def finish(i, summed, largest, total):
        if last:
            result = (summed / total).astype(jnp.bfloat16)
            for h in range(group):
                outs[0][pl.ds(i * run, run), h * HEAD_DIM : (h + 1) * HEAD_DIM] = result[
                    h * run : (h + 1) * run
                ]
        else:
            outs[0][pl.ds(i * tall, tall), :] = summed
            outs[1][pl.ds(i * tall, tall), :] = pack_state(largest, total, tall)

    @pl.when(count == 0)
    def _():
        for i in range(runs):
            state = state_in[i * tall : (i + 1) * tall, :]
            finish(i, summed_in[i * tall : (i + 1) * tall, :], state[:, :1], state[:, half : half + 1])

    @pl.when(count > 0)
    def _():
        for i in range(runs):
            q = stack_heads(q_ref, i * run, run)
            packed = state_in[i * tall : (i + 1) * tall, :]

            def step(block, carry, q=q):
                summed, largest, total = carry
                score = scores(q, kv_ref[block, :, :HEAD_DIM])
                new_largest = jnp.maximum(largest, jnp.max(score, axis=1, keepdims=True))
                fade = jnp.exp2((largest - new_largest) * SCALE)
                added, weight = weigh(score, new_largest)
                summed = summed * fade + jnp.dot(
                    weight, kv_ref[block, :, HEAD_DIM:], preferred_element_type=jnp.float32
                )
                return summed, new_largest, total * fade + added

            carry = (
                summed_in[i * tall : (i + 1) * tall, :],
                packed[:, :1],
                packed[:, half : half + 1],
            )
            if kv_ref.shape[0] == 1:
                carry = step(0, carry)
            else:
                carry = lax.fori_loop(0, count, step, carry)
            finish(i, *carry)


def attend_own(core, queries, own, other, run):
    rows, width = queries.shape
    tall = rows * (width // HEAD_DIM)
    whole = pl.BlockSpec(memory_space=pltpu.VMEM)
    shape = jax.ShapeDtypeStruct((tall, HEAD_DIM), jnp.float32)
    work = tall * rows
    return pl.pallas_call(
        functools.partial(own_kernel, run=run),
        in_specs=[pl.BlockSpec(memory_space=pltpu.SMEM), whole, whole, whole],
        out_specs=(whole, whole),
        out_shape=(shape, shape),
        compiler_params=pltpu.CompilerParams(vmem_limit_bytes=VMEM_LIMIT),
        cost_estimate=pl.CostEstimate(
            flops=8 * work * HEAD_DIM, transcendentals=2 * work, bytes_accessed=4 * tall * HEAD_DIM
        ),
        name="attend_own",
    )(core, queries, own, other)


def attend_earlier(count, queries, kv, summed, state, run, last):
    rows, width = queries.shape
    tall = rows * (width // HEAD_DIM)
    whole = pl.BlockSpec(memory_space=pltpu.VMEM)
    if last:
        shape = jax.ShapeDtypeStruct((rows, width), jnp.bfloat16)
    else:
        shape = (jax.ShapeDtypeStruct((tall, HEAD_DIM), jnp.float32),) * 2
    work = tall * kv.shape[0] * kv.shape[1]
    out = pl.pallas_call(
        functools.partial(earlier_kernel, run=run, last=last),
        in_specs=[pl.BlockSpec(memory_space=pltpu.SMEM), whole, whole, whole, whole],
        out_specs=whole if last else (whole, whole),
        out_shape=shape,
        compiler_params=pltpu.CompilerParams(vmem_limit_bytes=VMEM_LIMIT),
        cost_estimate=pl.CostEstimate(
            flops=4 * work * HEAD_DIM, transcendentals=work, bytes_accessed=4 * tall * HEAD_DIM
        ),
        name="attend_last" if last else "attend_earlier",
    )(count, queries, kv, summed, state)
    return out


def on_device(queries, keys, values, *, outer, groups, run):
    rows = queries.shape[0]
    scalar = lambda name: lax.axis_index(name).reshape(1).astype(jnp.int32)
    core, place = scalar("core"), scalar("outer")
    paired = jnp.concatenate(
        [keys.reshape(rows, groups, -1), values.reshape(rows, groups, -1)], axis=2
    ).reshape(rows, -1)
    axes = ("inner", "head")
    swap = [(0, 1), (1, 0)]
    own = lax.all_to_all(paired, axes, split_axis=1, concat_axis=0, tiled=True)
    q_own = lax.all_to_all(queries, axes, split_axis=1, concat_axis=0, tiled=True)
    if outer == 2:
        far = lax.ppermute(own, "outer", [(0, 1)])
        other = lax.ppermute(own, "core", swap)
        summed, state = attend_own(core, q_own, own, other, run)
        far, summed, state = lax.optimization_barrier((far, summed, state))
        far_other = lax.ppermute(far, "core", swap)
        summed, state = attend_earlier(place, q_own, far[None], summed, state, run, False)
        out = attend_earlier(place, q_own, far_other[None], summed, state, run, True)
    else:
        other = lax.ppermute(own, "core", swap)
        summed, state = attend_own(core, q_own, own, other, run)
        everything = lax.all_gather(own, ("outer", "core"), axis=0)
        out = attend_earlier(2 * place, q_own, everything, summed, state, run, True)
    return lax.all_to_all(out, axes, split_axis=0, concat_axis=1, tiled=True)


def solution(mesh):
    def run(queries, keys, values):
        head, seq = mesh.shape["head"], mesh.shape["seq"]
        inner = math.gcd(seq // 2, max(1, keys.shape[1] // HEAD_DIM // head))
        outer = seq // (2 * inner)
        split = Mesh(
            mesh.devices.reshape(head, outer, inner, 2), ("head", "outer", "inner", "core")
        )
        spec = P(("outer", "inner", "core", "head"), None)
        return jax.shard_map(
            functools.partial(
                on_device,
                outer=outer,
                groups=head * inner,
                run=queries.shape[0] // (seq * head) * head,
            ),
            mesh=split,
            in_specs=(spec, spec, spec),
            out_specs=spec,
            check_vma=False,
        )(queries, keys, values)

    return run
```

```python
import functools
import math

import jax
import jax.numpy as jnp
from jax import lax
from jax.experimental import pallas as pl
from jax.experimental.pallas import tpu as pltpu
from jax.sharding import Mesh, PartitionSpec as P


HEAD_DIM = 128
SCALE = math.log2(math.e) / math.sqrt(HEAD_DIM)
DIMS_NT = (((1,), (1,)), ((), ()))
VMEM_LIMIT = 24 * 1024 * 1024


def scores(q, k):
    return lax.dot_general(q, k, DIMS_NT, preferred_element_type=jnp.float32)


def weigh(score, largest):
    weight = jnp.exp2((score - largest) * SCALE)
    return jnp.sum(weight, axis=1, keepdims=True), weight.astype(jnp.bfloat16)


def stack_heads(ref, start, rows):
    group = ref.shape[1] // HEAD_DIM
    return jnp.concatenate(
        [ref[pl.ds(start, rows), h * HEAD_DIM : (h + 1) * HEAD_DIM] for h in range(group)], axis=0
    )


def pack_kernel(key_ref, value_ref, out_ref):
    groups, _, width = out_ref.shape
    half = width // 2
    for g in range(groups):
        out_ref[g, :, :half] = key_ref[:, g * half : (g + 1) * half]
        out_ref[g, :, half:] = value_ref[:, g * half : (g + 1) * half]


def pack(keys, values, groups):
    rows, width = keys.shape
    whole = pl.BlockSpec(memory_space=pltpu.VMEM)
    return pl.pallas_call(
        pack_kernel,
        in_specs=[whole, whole],
        out_specs=whole,
        out_shape=jax.ShapeDtypeStruct((groups, rows, 2 * width // groups), keys.dtype),
        name="pack",
    )(keys, values)


def spread(column, like):
    return jnp.broadcast_to(column, like.shape)


def own_kernel(core_ref, q_ref, own_ref, other_ref, summed_ref, largest_ref, total_ref, *, run):
    group = q_ref.shape[1] // HEAD_DIM
    tall = group * run
    row = lax.broadcasted_iota(jnp.int32, (tall, run), 0) % run
    col = lax.broadcasted_iota(jnp.int32, (tall, run), 1)
    low = jnp.float32(-1e30)
    see_other = lax.broadcast(core_ref[0], (tall, run)) > 0
    for i in range(q_ref.shape[0] // run):
        q = stack_heads(q_ref, i * run, run)
        own = scores(q, own_ref[: (i + 1) * run, :HEAD_DIM])
        other = scores(q, other_ref[: (i + 1) * run, :HEAD_DIM])
        own_edge = jnp.where(col <= row, own[:, i * run :], low)
        other_edge = jnp.where(see_other, other[:, i * run :], low)
        if i:
            own_edge = jnp.concatenate([own[:, : i * run], own_edge], axis=1)
            other_edge = jnp.concatenate([other[:, : i * run], other_edge], axis=1)
        largest = jnp.maximum(
            jnp.max(own_edge, axis=1, keepdims=True), jnp.max(other_edge, axis=1, keepdims=True)
        )
        own_total, own_weight = weigh(own_edge, largest)
        other_total, other_weight = weigh(other_edge, largest)
        summed_ref[i * tall : (i + 1) * tall, :] = jnp.dot(
            own_weight, own_ref[: (i + 1) * run, HEAD_DIM:], preferred_element_type=jnp.float32
        ) + jnp.dot(
            other_weight, other_ref[: (i + 1) * run, HEAD_DIM:], preferred_element_type=jnp.float32
        )
        shape = (tall, HEAD_DIM)
        largest_ref[i * tall : (i + 1) * tall, :] = jnp.broadcast_to(largest, shape)
        total_ref[i * tall : (i + 1) * tall, :] = jnp.broadcast_to(own_total + other_total, shape)


def earlier_kernel(count_ref, q_ref, kv_ref, *refs, run, last):
    group = q_ref.shape[1] // HEAD_DIM
    tall = group * run
    runs = q_ref.shape[0] // run
    repeats = kv_ref.shape[1] // HEAD_DIM
    count = count_ref[0]
    given, outs = refs[:3], refs[3:]

    def finish(i, carry):
        if last:
            result = (carry[0] / carry[2]).astype(jnp.bfloat16)
            for h in range(group):
                outs[0][pl.ds(i * run, run), h * HEAD_DIM : (h + 1) * HEAD_DIM] = result[
                    h * run : (h + 1) * run
                ]
        else:
            for ref, value in zip(outs, carry):
                ref[i * tall : (i + 1) * tall, :] = value

    def load(i):
        return tuple(ref[i * tall : (i + 1) * tall, :] for ref in given)

    @pl.when(count == 0)
    def _():
        for i in range(runs):
            finish(i, load(i))

    @pl.when(count > 0)
    def _():
        for i in range(runs):
            q = stack_heads(q_ref, i * run, run)

            def step(block, carry, q=q):
                summed, largest, total = carry
                score = scores(q, kv_ref[block, :, :HEAD_DIM])
                new_largest = jnp.maximum(
                    largest, spread(jnp.max(score, axis=1, keepdims=True), largest)
                )
                fade = jnp.exp2((largest - new_largest) * SCALE)
                added, weight = weigh(score, jnp.concatenate([new_largest] * repeats, axis=1))
                summed = summed * fade + jnp.dot(
                    weight, kv_ref[block, :, HEAD_DIM:], preferred_element_type=jnp.float32
                )
                return summed, new_largest, total * fade + spread(added, total)

            if kv_ref.shape[0] == 1:
                carry = step(0, load(i))
            else:
                carry = lax.fori_loop(0, count, step, load(i))
            finish(i, carry)


def attend_own(core, queries, own, other, run):
    rows, width = queries.shape
    tall = rows * (width // HEAD_DIM)
    whole = pl.BlockSpec(memory_space=pltpu.VMEM)
    shape = jax.ShapeDtypeStruct((tall, HEAD_DIM), jnp.float32)
    work = tall * rows
    return pl.pallas_call(
        functools.partial(own_kernel, run=run),
        in_specs=[pl.BlockSpec(memory_space=pltpu.SMEM), whole, whole, whole],
        out_specs=(whole,) * 3,
        out_shape=(shape,) * 3,
        compiler_params=pltpu.CompilerParams(vmem_limit_bytes=VMEM_LIMIT),
        cost_estimate=pl.CostEstimate(
            flops=8 * work * HEAD_DIM, transcendentals=2 * work, bytes_accessed=4 * tall * HEAD_DIM
        ),
        name="attend_own",
    )(core, queries, own, other)


def attend_earlier(count, queries, kv, state, run, last):
    rows, width = queries.shape
    tall = rows * (width // HEAD_DIM)
    whole = pl.BlockSpec(memory_space=pltpu.VMEM)
    if last:
        shape = jax.ShapeDtypeStruct((rows, width), jnp.bfloat16)
    else:
        shape = (jax.ShapeDtypeStruct((tall, HEAD_DIM), jnp.float32),) * 3
    work = tall * kv.shape[0] * kv.shape[1]
    out = pl.pallas_call(
        functools.partial(earlier_kernel, run=run, last=last),
        in_specs=[pl.BlockSpec(memory_space=pltpu.SMEM)] + [whole] * 5,
        out_specs=whole if last else (whole,) * 3,
        out_shape=shape,
        compiler_params=pltpu.CompilerParams(vmem_limit_bytes=VMEM_LIMIT),
        cost_estimate=pl.CostEstimate(
            flops=4 * work * HEAD_DIM, transcendentals=work, bytes_accessed=4 * tall * HEAD_DIM
        ),
        name="attend_last" if last else "attend_earlier",
    )(count, queries, kv, *state)
    return out


def on_device(queries, keys, values, *, outer, groups, run):
    rows = queries.shape[0]
    scalar = lambda name: lax.axis_index(name).reshape(1).astype(jnp.int32)
    core, place = scalar("core"), scalar("outer")
    axes = ("inner", "head")
    swap = [(0, 1), (1, 0)]
    own = lax.all_to_all(pack(keys, values, groups), axes, split_axis=0, concat_axis=0, tiled=True)
    own = own.reshape(groups * rows, -1)
    q_own = lax.all_to_all(queries, axes, split_axis=1, concat_axis=0, tiled=True)
    other = lax.ppermute(own, "core", swap)
    if outer == 2:
        far = lax.ppermute(own, "outer", [(0, 1)])
        far_other = lax.ppermute(far, "core", swap)
        state = attend_own(core, q_own, own, other, run)
        state = attend_earlier(place, q_own, far[None], state, run, False)
        out = attend_earlier(place, q_own, far_other[None], state, run, True)
    else:
        state = attend_own(core, q_own, own, other, run)
        everything = lax.all_gather(own, ("outer", "core"), axis=0)
        out = attend_earlier(2 * place, q_own, everything, state, run, True)
    return lax.all_to_all(out, axes, split_axis=0, concat_axis=1, tiled=True)


def solution(mesh):
    def run(queries, keys, values):
        head, seq = mesh.shape["head"], mesh.shape["seq"]
        inner = math.gcd(seq // 2, max(1, keys.shape[1] // HEAD_DIM // head))
        outer = seq // (2 * inner)
        split = Mesh(
            mesh.devices.reshape(head, outer, inner, 2), ("head", "outer", "inner", "core")
        )
        spec = P(("outer", "inner", "core", "head"), None)
        body = functools.partial(
            on_device,
            outer=outer,
            groups=head * inner,
            run=queries.shape[0] // (seq * head) * head,
        )

        return jax.shard_map(
            body,
            mesh=split,
            in_specs=(spec, spec, spec),
            out_specs=spec,
            check_vma=False,
        )(queries, keys, values)

    return run
```
